256 devices in a mesh: rows: 256 (over x, y, z, core).
Axes of the slice: x: 4, y: 4, z: 8, core: 2. Of those that a mesh axis runs over, the one named last changes fastest.
Arguments:
- q_final: float32 [393216, 512], P('rows'), may hold values from -0.050370466 to 0.050370466
- r_first: float32 [512, 512], replicated, may hold values from -1 to 2, as said below
- r_second: float32 [512, 512], replicated, may hold values from -1 to 2, as said below
- q_grad: float32 [393216, 512], P('rows'), may hold values from -6 to 6
- r_grad: float32 [512, 512], replicated, may hold values from -1.5 to 1.5
Outputs:
- a_grad: float32 [393216, 512], P('rows')
The draws below stay inside these ranges and needn't reach their ends.
Inputs may be any that keep to these rules, and one draw needn't show every extreme that they name: `r_first`: upper triangular, diagonal between 1 and 2. `r_second`: upper triangular, diagonal between 1 and 2.
All inputs are finite; a program needn't handle non-finite values.
Results may differ from the reference program's by a relative error of at most 0.000084.
Values sent between devices are 32-bit elements; how exact they have to be, the bound alone decides.
A program may use at most 128 MiB of HBM per device.

```python
import math
import jax
import jax.numpy as jnp
from jax import lax

W = 512
TOTAL = 393216


def triangle(key, salt):
    folded = jax.random.fold_in(key, salt)
    key_diag, key_off = jax.random.split(folded)
    diagonal = jnp.exp(jax.random.uniform(key_diag, (W,), jnp.float32, 0.0, math.log(2.0)))
    offdiag = jax.random.normal(key_off, (W, W), jnp.float32) * (0.25 / math.sqrt(W))
    return jnp.triu(offdiag, 1) + jnp.diag(diagonal)


def draw_r_first(key, part):
    return triangle(key, 11)


def draw_r_second(key, part):
    return triangle(key, 23)


def shard_levels(own_key, extent, cuts, smallest, top_value):
    factor_of, own = 1.0, jax.random.fold_in(own_key, 6)
    for position, blocks in cuts:
        draws = jnp.exp(jax.random.uniform(jax.random.fold_in(own, position), (blocks,), jnp.float32, smallest / len(cuts), top_value / len(cuts)))
        factor_of = factor_of * jnp.repeat(draws, extent[position] // blocks).reshape([-1 if axis == position else 1 for axis in range(len(extent))])
    return factor_of


def noise(key, extent, width, limit, cuts=(), held_as=jnp.bfloat16):
    result = width * jax.random.normal(key, extent, jnp.float32)
    if cuts:
        result = result * shard_levels(key, extent, cuts, -0.22, 0.18)
    return jnp.clip(result, -limit, limit).astype(held_as)


def setup_inputs(seed: int = 0) -> dict:
    key_of = jax.random.split(jax.random.key(seed), 6)
    q_final = noise(key_of[0], (TOTAL, W), ((TOTAL * W) ** -0.25), 0.050370466, ((0, 256),), jnp.float32)
    r_first = draw_r_first(jax.random.fold_in(key_of[5], 71), 0)
    r_second = draw_r_second(jax.random.fold_in(key_of[5], 71), 0)
    q_grad = noise(key_of[3], (TOTAL, W), 1.0, 6.0, ((0, 256),), jnp.float32)
    r_grad = noise(key_of[4], (W, W), 0.25, 1.5, (), jnp.float32)
    return {"q_final": q_final, "r_first": r_first, "r_second": r_second, "q_grad": q_grad, "r_grad": r_grad}


HIGHEST = lax.Precision.HIGHEST

def copy_lower(matrix):
    return jnp.tril(matrix) + jnp.tril(matrix, -1).T

def right_solve(left, upper):
    return lax.linalg.triangular_solve(upper, left, left_side=False, lower=False, transpose_a=True)

def reference(q_final, r_first, r_second, q_grad, r_grad):
    q_first = jnp.dot(q_final, r_second, precision=HIGHEST)
    grad_second = jnp.dot(r_grad, r_first.T, precision=HIGHEST)
    grad_first = jnp.dot(r_second.T, r_grad, precision=HIGHEST)
    mix_second = jnp.dot(r_second, grad_second.T, precision=HIGHEST) - jnp.dot(q_grad.T, q_final, precision=HIGHEST)
    inner = q_grad + jnp.dot(q_final, copy_lower(mix_second), precision=HIGHEST)
    q_first_grad = right_solve(inner, r_second)
    mix_first = jnp.dot(r_first, grad_first.T, precision=HIGHEST) - jnp.dot(q_first_grad.T, q_first, precision=HIGHEST)
    outer = q_first_grad + jnp.dot(q_first, copy_lower(mix_first), precision=HIGHEST)
    return right_solve(outer, r_first)
```

```python
import jax
import jax.numpy as jnp
from jax import lax
from jax.experimental import pallas as pl
from jax.experimental.pallas import tpu as pltpu
from jax.sharding import PartitionSpec as P

HIGHEST = lax.Precision.HIGHEST
W, HALF = 512, 256
NX, NY, NZ = 4, 4, 8
SPLIT = 5
NN, NT, TN = ((1,), (0,)), ((1,), (1,)), ((0,), (0,))


def mm(a, b, precision=HIGHEST, dims=NN):
    return lax.dot_general(a, b, (dims, ((), ())), precision=precision, preferred_element_type=jnp.float32)


def halves(a):
    high = a.astype(jnp.bfloat16)
    return high, (a - high.astype(jnp.float32)).astype(jnp.bfloat16)


def mm3(a, b, dims=NN):
    ah, al = a if isinstance(a, tuple) else halves(a)
    bh, bl = b if isinstance(b, tuple) else halves(b)

    def dot(u, v):
        return lax.dot_general(u, v, (dims, ((), ())), preferred_element_type=jnp.float32)

    return dot(ah, bh) + (dot(ah, bl) + dot(al, bh))


def iotas(rows, cols):
    return lax.broadcasted_iota(jnp.int32, (rows, cols), 0), lax.broadcasted_iota(jnp.int32, (rows, cols), 1)


def gram_step(g, q):
    gs, qs = halves(g), halves(q)
    left = mm3(
        tuple(jnp.concatenate([a, b[:, :HALF]], axis=1) for a, b in zip(gs, qs)), tuple(b[:, :HALF] for b in qs), TN
    )
    right = mm3(
        tuple(jnp.concatenate([a[:, HALF:], b], axis=1) for a, b in zip(gs, qs)), tuple(b[:, HALF:] for b in qs), TN
    )
    return left, right


def pack(left, right, packed):
    row, col = iotas(HALF, HALF)
    low, eye = row >= col, row == col
    square = (
        (jnp.where(low, left[:HALF], left[2 * HALF :]), right[HALF : 2 * HALF]),
        (left[HALF : 2 * HALF], jnp.where(low, right[:HALF], right[2 * HALF :])),
    )
    diag = [jnp.sum(jnp.where(eye, m[2 * HALF :], 0.0), axis=0, keepdims=True) for m in (left, right)]
    first = lax.broadcasted_iota(jnp.int32, (8, 128), 0) == 0
    for group in range(32):
        for tile in range(8):
            r, l = group * 16 + (tile // 4) * 8, (tile % 4) * 128
            part = square[r // HALF][l // HALF]
            packed[group // 16, (group // 4) % 4, group % 4, tile] = part[r % HALF : r % HALF + 8, l % HALF : l % HALF + 128]
        extra = jnp.zeros((8, 128), jnp.float32)
        if group < 4:
            line = diag[group // 2][:, (group % 2) * 128 : (group % 2) * 128 + 128]
            extra = jnp.where(first, jnp.broadcast_to(line, (8, 128)), 0.0)
        packed[group // 16, (group // 4) % 4, group % 4, 8] = extra


def unpack(packed, square, diag):
    for group in range(32):
        at = (group // 16, (group // 4) % 4, group % 4)
        for tile in range(8):
            r, l = group * 16 + (tile // 4) * 8, (tile % 4) * 128
            square[r : r + 8, l : l + 128] = packed[(*at, tile)]
        if group < 4:
            diag[:, group * 128 : group * 128 + 128] = packed[(*at, 8)]


def gram_kernel(g_ref, q_ref, packed, acc):
    step = pl.program_id(0)
    left, right = gram_step(g_ref[...], q_ref[...])

    @pl.when(step == 0)
    def _():
        acc[0], acc[1] = left, right

    @pl.when(step > 0)
    def _():
        acc[0] += left
        acc[1] += right

    @pl.when(step == pl.num_programs(0) - 1)
    def _():
        pack(acc[0], acc[1], packed)


def gram(q_grad, q_final):
    rows = q_grad.shape[0] // 3
    spec = pl.BlockSpec((rows, W), lambda i: (i, 0))
    return pl.pallas_call(
        gram_kernel,
        grid=(3,),
        in_specs=[spec, spec],
        out_specs=pl.BlockSpec((2, NX, NY, 9, 8, 128), lambda i: (0, 0, 0, 0, 0, 0)),
        out_shape=jax.ShapeDtypeStruct((2, NX, NY, 9, 8, 128), jnp.float32),
        scratch_shapes=[pltpu.VMEM((2, 3 * HALF, HALF), jnp.float32)],
        compiler_params=pltpu.CompilerParams(vmem_limit_bytes=48 << 20),
        name="gram",
    )(q_grad, q_final)


def inverse_blocks(upper_refs, out_refs, size=128):
    row, col = iotas(size, size)
    eye, above = row == col, col > row
    where = [(m, b) for m in range(len(upper_refs)) for b in range(W // size)]
    block = [upper_refs[m][b * size : b * size + size, b * size : b * size + size] for m, b in where]
    inv = []
    for u in block:
        d_row = 1.0 / jnp.sum(jnp.where(eye, u, 0.0), axis=0, keepdims=True)
        d_col = 1.0 / jnp.sum(jnp.where(eye, u, 0.0), axis=1, keepdims=True)
        pair = above & (row // 2 == col // 2)
        inv.append(jnp.where(eye, d_row, jnp.where(pair, -(u * d_col) * d_row, 0.0)))
    s = 2
    while s < size:
        between = above & (row // (2 * s) == col // (2 * s)) & (row // s != col // s)
        half = [mm(jnp.where(between, u, 0.0), x, HIGHEST) for u, x in zip(block, inv)]
        inv = [x - mm(x, h, HIGHEST) for x, h in zip(inv, half)]
        s *= 2
    for ref in out_refs:
        ref[...] = jnp.zeros((W, W), jnp.float32)
    for (m, b), x in zip(where, inv):
        out_refs[m][b * size : b * size + size, b * size : b * size + size] = x
    while s < W:
        for m in range(len(upper_refs)):
            for b in range(0, W, 2 * s):
                top, low = slice(b, b + s), slice(b + s, b + 2 * s)
                h = mm(upper_refs[m][top, low], out_refs[m][low, low], HIGHEST)
                out_refs[m][top, low] = -mm(out_refs[m][top, top], h, HIGHEST)
        s *= 2


def prep_kernel(r1, r2, rg, inv1, inv2, both, k1, k2):
    t = mm(r1[...], rg[...], HIGHEST, NT)
    k2[...] = mm(r2[...], t, HIGHEST)
    k1[...] = mm(t, r2[...], HIGHEST)
    inverse_blocks((r1, r2), (inv1, inv2))
    both[...] = mm(inv1[...], inv2[...], HIGHEST)


def prep(r_first, r_second, r_grad):
    vmem = pl.BlockSpec(memory_space=pltpu.VMEM)
    return pl.pallas_call(
        prep_kernel,
        in_specs=[vmem] * 3,
        out_specs=[vmem] * 5,
        out_shape=[jax.ShapeDtypeStruct((W, W), jnp.float32)] * 5,
        compiler_params=pltpu.CompilerParams(vmem_limit_bytes=48 << 20),
        name="prep",
    )(r_first, r_second, r_grad)


def place():
    me = lax.axis_index("rows")
    c = lax.rem(me, 2)
    z = lax.rem(lax.div(me, 2), NZ)
    y = lax.rem(lax.div(me, 2 * NZ), NY)
    x = lax.div(me, 2 * NZ * NY)
    return x, y, z, c


def device(x, y, z, c):
    return (((x * NY + y) * NZ + z) * 2 + c,)


def exchange_kernel(packed, square, diag, *scratch):
    (core_in, mine, a1_in, b1_in, a2, b2, a2_in, b2_in, own, z_in, whole, s_core, r_core, s_a1, r_a1, s_b1, r_b1, s_a2,
     r_a2, s_b2, r_b2, s_z, r_z, s_a3, r_a3, s_b3, r_b3, s_a4, r_a4, s_b4, r_b4, s_last, r_last) = scratch
    x, y, z, c = place()
    other = device(x, y, z, 1 - c)
    xs = [lax.rem(x + k, NX) for k in range(1, NX)]
    ys = [lax.rem(y + k, NY) for k in range(1, NY)]
    zs = [lax.rem(z + k, NZ) for k in range(1, NZ)]
    to_x = [device(p, y, z, c) for p in xs]
    to_y = [device(x, p, z, c) for p in ys]
    to_z = [device(x, y, p, c) for p in zs]

    barrier = pltpu.get_barrier_semaphore()
    peers = [other, *to_x, *to_y, *to_z]
    for peer in peers:
        pl.semaphore_signal(barrier, inc=1, device_id=peer, device_id_type=pl.DeviceIdType.MESH)
    pl.semaphore_wait(barrier, len(peers))

    def send(src, dst, sems, k, to):
        copy = pltpu.make_async_remote_copy(src_ref=src, dst_ref=dst, send_sem=sems[0].at[k], recv_sem=sems[1].at[k],
                                            device_id=to, device_id_type=pl.DeviceIdType.MESH)
        copy.start()
        return copy

    started = []
    copy = send(packed.at[1 - c], core_in, (s_core, r_core), 0, other)
    started.append(copy)
    copy.wait_recv()
    mine[...] = packed[c] + core_in[...]
    one_a = [send(mine.at[xs[k], :, pl.ds(0, SPLIT)], a1_in.at[k], (s_a1, r_a1), k, to_x[k]) for k in range(3)]
    one_b = [send(mine.at[:, ys[k], pl.ds(SPLIT, 9 - SPLIT)], b1_in.at[k], (s_b1, r_b1), k, to_y[k]) for k in range(3)]
    for copy in one_a:
        copy.wait_recv()
    a2[...] = (mine[x, :, 0:SPLIT] + a1_in[0]) + (a1_in[1] + a1_in[2])
    two_a = [send(a2.at[ys[k]], a2_in.at[k], (s_a2, r_a2), k, to_y[k]) for k in range(3)]
    for copy in one_b:
        copy.wait_recv()
    b2[...] = (mine[:, y, SPLIT:9] + b1_in[0]) + (b1_in[1] + b1_in[2])
    two_b = [send(b2.at[xs[k]], b2_in.at[k], (s_b2, r_b2), k, to_x[k]) for k in range(3)]
    for copy in two_a:
        copy.wait_recv()
    own[0:SPLIT] = (a2[y] + a2_in[0]) + (a2_in[1] + a2_in[2])
    for copy in two_b:
        copy.wait_recv()
    own[SPLIT:9] = (b2[x] + b2_in[0]) + (b2_in[1] + b2_in[2])
    three = [send(own, z_in.at[k], (s_z, r_z), k, to_z[k]) for k in range(NZ - 1)]
    total = own[...]
    for k, copy in enumerate(three):
        copy.wait_recv()
        total = total + z_in[k]
    whole[c, x, y] = total
    at_a, at_b = whole.at[c, x, y, pl.ds(0, SPLIT)], whole.at[c, x, y, pl.ds(SPLIT, 9 - SPLIT)]
    four_a = [send(at_a, at_a, (s_a3, r_a3), k, to_y[k]) for k in range(3)]
    four_b = [send(at_b, at_b, (s_b3, r_b3), k, to_x[k]) for k in range(3)]
    for copy in four_a:
        copy.wait_recv()
    line_a = whole.at[c, x, :, pl.ds(0, SPLIT)]
    five_a = [send(line_a, line_a, (s_a4, r_a4), k, to_x[k]) for k in range(3)]
    for copy in four_b:
        copy.wait_recv()
    line_b = whole.at[c, :, y, pl.ds(SPLIT, 9 - SPLIT)]
    five_b = [send(line_b, line_b, (s_b4, r_b4), k, to_y[k]) for k in range(3)]
    for copy in (*five_a, *five_b):
        copy.wait_recv()
    last = send(whole.at[c], whole.at[c], (s_last, r_last), 0, other)
    last.wait_recv()
    for copy in (*started, *one_a, *one_b, *two_a, *two_b, *three, *four_a, *four_b, *five_a, *five_b, last):
        copy.wait_send()
    unpack(whole, square, diag)


def exchange_scratch():
    f32, a, b = jnp.float32, SPLIT, 9 - SPLIT
    shapes = [(NX, NY, 9), (NX, NY, 9), (3, NY, a), (3, NX, b), (NY, a), (NX, b), (3, a), (3, b), (9,), (NZ - 1, 9), (2, NX, NY, 9)]
    counts = [1, 3, 3, 3, 3, NZ - 1, 3, 3, 3, 3, 1]
    sems = [pltpu.SemaphoreType.DMA((n,)) for n in counts for _ in range(2)]
    return [pltpu.VMEM((*s, 8, 128), f32) for s in shapes] + sems


def exchange(packed):
    vmem = pl.BlockSpec(memory_space=pltpu.VMEM)
    return pl.pallas_call(
        exchange_kernel,
        in_specs=[vmem],
        out_specs=[vmem, vmem],
        out_shape=[jax.ShapeDtypeStruct((W, W), jnp.float32), jax.ShapeDtypeStruct((8, W), jnp.float32)],
        scratch_shapes=exchange_scratch(),
        compiler_params=pltpu.CompilerParams(collective_id=0, has_side_effects=True, vmem_limit_bytes=32 << 20),
        name="exchange",
    )(packed)


def copy_lower(m, low, strict):
    return jnp.where(low, m, 0.0) + jnp.where(strict, m, 0.0).T


def middle(square, diag, r2, inv1, inv2, both, k1, k2):
    row, col = iotas(W, W)
    low, strict, eye = row >= col, row > col, row == col
    upper = jnp.where(row < col, square, 0.0)
    gram_sum = upper + upper.T + jnp.where(eye, jnp.broadcast_to(diag, (W, W)), 0.0)
    cross = jnp.where(low, square, 0.0)
    second = copy_lower(k2 - square, low, strict)
    second_halves, r2_halves = halves(second), halves(r2)
    solved = mm3(inv2, mm3(cross + mm3(second_halves, gram_sum), r2_halves))
    first = copy_lower(k1 - solved, low, strict)
    return mm3(second_halves, both, NT) + mm3(r2_halves, mm3(first, inv1, NT))


def middle_kernel(square, diag, r2, inv1, inv2, both, k1, k2, out):
    out[...] = middle(square[...], diag[0:1], r2[...], inv1[...], inv2[...], both[...], k1[...], k2[...])


def middle_call(*args):
    vmem = pl.BlockSpec(memory_space=pltpu.VMEM)
    return pl.pallas_call(
        middle_kernel,
        in_specs=[vmem] * 8,
        out_specs=vmem,
        out_shape=jax.ShapeDtypeStruct((W, W), jnp.float32),
        compiler_params=pltpu.CompilerParams(vmem_limit_bytes=48 << 20),
        name="middle",
    )(*args)


def finish_kernel(g, q, both, last, out):
    out[...] = mm3(g[...], both[...], NT) + mm3(q[...], last[...])


def finish(q_grad, q_final, both, last):
    rows = q_grad.shape[0] // 6
    spec = pl.BlockSpec((rows, W), lambda i: (i, 0))
    small = pl.BlockSpec((W, W), lambda i: (0, 0))
    return pl.pallas_call(
        finish_kernel,
        grid=(6,),
        in_specs=[spec, spec, small, small],
        out_specs=spec,
        out_shape=jax.ShapeDtypeStruct(q_grad.shape, jnp.float32),
        compiler_params=pltpu.CompilerParams(vmem_limit_bytes=48 << 20),
        name="finish",
    )(q_grad, q_final, both, last)


def local(q_final, r_first, r_second, q_grad, r_grad):
    inv1, inv2, both, k1, k2 = prep(r_first, r_second, r_grad)
    square, diag = exchange(gram(q_grad, q_final))
    last = middle_call(square, diag, r_second, inv1, inv2, both, k1, k2)
    return finish(q_grad, q_final, both, last)


def solution(mesh):
    placed = (P("rows", None), P(), P(), P("rows", None), P())
    return jax.shard_map(local, mesh=mesh, in_specs=placed, out_specs=P("rows", None), check_vma=False)
```

```python
import jax
import jax.numpy as jnp
from jax import lax
from jax.experimental import pallas as pl
from jax.experimental.pallas import tpu as pltpu
from jax.sharding import PartitionSpec as P

HIGHEST = lax.Precision.HIGHEST
W, HALF = 512, 256
NX, NY, NZ = 4, 4, 8
ROWS, STEPS = 1536, 3
PARTS = ((0, 5, True), (5, 4, False))
NN, NT, TN = ((1,), (0,)), ((1,), (1,)), ((0,), (0,))
A, B = slice(0, HALF), slice(HALF, W)


def mm(a, b):
    return lax.dot_general(a, b, (NN, ((), ())), precision=HIGHEST, preferred_element_type=jnp.float32)


def halves(a):
    high = a.astype(jnp.bfloat16)
    return high, (a - high.astype(jnp.float32)).astype(jnp.bfloat16)


def cut(pair, *index):
    return pair[0][index], pair[1][index]


def join(pairs, axis):
    return tuple(jnp.concatenate([p[i] for p in pairs], axis=axis) for i in range(2))


def mm3(a, b, dims=NN):
    (ah, al), (bh, bl) = a, b

    def dot(u, v):
        return lax.dot_general(u, v, (dims, ((), ())), preferred_element_type=jnp.float32)

    return dot(ah, bh) + (dot(ah, bl) + dot(al, bh))


def iotas(rows, cols):
    return lax.broadcasted_iota(jnp.int32, (rows, cols), 0), lax.broadcasted_iota(jnp.int32, (rows, cols), 1)


def small_inverses(uppers, size=128):
    row, col = iotas(size, size)
    eye, above = row == col, col > row
    block = [u[b : b + size, b : b + size] for u in uppers for b in range(0, W, size)]
    inv = []
    for u in block:
        d_row = 1.0 / jnp.sum(jnp.where(eye, u, 0.0), axis=0, keepdims=True)
        d_col = 1.0 / jnp.sum(jnp.where(eye, u, 0.0), axis=1, keepdims=True)
        pair = above & (row // 2 == col // 2)
        inv.append(jnp.where(eye, d_row, jnp.where(pair, -(u * d_col) * d_row, 0.0)))
    s = 2
    while s < size:
        between = above & (row // (2 * s) == col // (2 * s)) & (row // s != col // s)
        half = [mm(jnp.where(between, u, 0.0), x) for u, x in zip(block, inv)]
        inv = [x - mm(x, h) for x, h in zip(inv, half)]
        s *= 2
    return inv


def join_inverses(uppers, outs, size=128):
    s = size
    while s < W:
        for u, out in zip(uppers, outs):
            for b in range(0, W, 2 * s):
                top, low = slice(b, b + s), slice(b + s, b + 2 * s)
                out[top, low] = -mm(out[top, top], mm(u[top, low], out[low, low]))
        s *= 2


def place():
    me = lax.axis_index("rows")
    c = lax.rem(me, 2)
    z = lax.rem(lax.div(me, 2), NZ)
    y = lax.rem(lax.div(me, 2 * NZ), NY)
    x = lax.div(me, 2 * NZ * NY)
    return x, y, z, c


def device(x, y, z, c):
    return (((x * NY + y) * NZ + z) * 2 + c,)


def pack_half(h, wide, square, put):
    row, col = iotas(HALF, HALF)
    low, eye = row >= col, row == col
    is_top = jnp.full((HALF, HALF), h, jnp.int32) == 0
    parts = (jnp.where(low & is_top, square, wide[:, A]), jnp.where(low | is_top, wide[:, B], square))
    diag = jnp.sum(jnp.where(eye, jnp.where(is_top, wide[:, A], square), 0.0), axis=0, keepdims=True)
    first = lax.broadcasted_iota(jnp.int32, (8, 128), 0) == 0
    for group in range(16):
        for tile in range(8):
            r, l = group * 16 + (tile // 4) * 8, (tile % 4) * 128
            put(group // 4, group % 4, tile, parts[l // HALF][r : r + 8, l % HALF : l % HALF + 128])
        extra = jnp.zeros((8, 128), jnp.float32)
        if group < 2:
            extra = jnp.where(first, jnp.broadcast_to(diag[:, group * 128 : group * 128 + 128], (8, 128)), 0.0)
        put(group // 4, group % 4, 8, extra)


def copy_lower(m, low, strict):
    return jnp.where(low, m, 0.0) + jnp.where(strict, m, 0.0).T


def symmetric(b00, b10, b11):
    row, col = iotas(HALF, HALF)
    low, strict = row >= col, row > col
    top = jnp.concatenate([copy_lower(b00, low, strict), b10.T], axis=1)
    return jnp.concatenate([top, jnp.concatenate([b10, copy_lower(b11, low, strict)], axis=1)], axis=0)


def middle(square, diag, k1, k2, r2, inv1, inv2, both):
    row, col = iotas(HALF, HALF)
    low, strict, above, eye = row >= col, row > col, row < col, row == col
    second = halves(symmetric(*(k2[i, j] - square[i, j] for i, j in ((A, A), (B, A), (B, B)))))
    grams = []
    for s in (A, B):
        upper = jnp.where(above, square[s, s], 0.0)
        grams.append(upper + upper.T + jnp.where(eye, jnp.broadcast_to(diag[:, s], (HALF, HALF)), 0.0))
    g01 = square[A, B]
    gram_a = halves(jnp.concatenate([grams[0], g01.T], axis=0))
    gram_b = halves(jnp.concatenate([g01, grams[1]], axis=0))
    cross_a = jnp.concatenate([jnp.where(low, square[A, A], 0.0), square[B, A]], axis=0)
    y_a = halves(cross_a + mm3(second, gram_a))
    y_bb = halves(jnp.where(low, square[B, B], 0.0) + mm3(cut(second, B), gram_b))
    w_a = halves(mm3(y_a, cut(r2, A, A)))
    w_bb = halves(mm3(join([cut(y_a, B), y_bb], 1), cut(r2, slice(None), B)))
    z_aa = mm3(cut(inv2, A), w_a)
    z_b = mm3(cut(inv2, B, B), join([cut(w_a, B), w_bb], 1))
    first = halves(symmetric(k1[A, A] - z_aa, k1[B, A] - z_b[:, A], k1[B, B] - z_b[:, B]))
    v = halves(times_lower(first, inv1))
    add = times_lower(second, both)
    return add[A] + mm3(cut(r2, A), v), add[B] + mm3(cut(r2, B, B), cut(v, B))


def times_lower(a, upper):
    return jnp.concatenate([mm3(a, cut(upper, A), NT), mm3(cut(a, slice(None), B), cut(upper, B, B), NT)], axis=1)


def main_kernel(q_hbm, r1_hbm, r2_hbm, g_hbm, rg_hbm, m2_out, u_hbm, *scratch):
    scratch = list(scratch)
    q_in, g_in, slab_h, slab_l, r1, r2, rg, inv1, inv2, k1, k2, u_buf, square, diag, acc = (scratch.pop(0) for _ in range(15))
    bf = [scratch.pop(0) for _ in range(8)]
    r2_p, inv1_p, inv2_p, both_p = (tuple(bf[i : i + 2]) for i in range(0, 8, 2))
    theirs, core_in, mine, own, z_in, whole = (scratch.pop(0) for _ in range(6))
    one_in, two, two_in = ([scratch.pop(0) for _ in PARTS] for _ in range(3))
    in_sem, u_sem, core_sem, one_sem, two_sem, z_sem, four_sem, five_sem, last_sem = (scratch.pop(0) for _ in range(9))
    x, y, z, c = place()
    other = device(x, y, z, 1 - c)
    xs = [lax.rem(x + k, NX) for k in range(1, NX)]
    ys = [lax.rem(y + k, NY) for k in range(1, NY)]
    to_x = [device(p, y, z, c) for p in xs]
    to_y = [device(x, p, z, c) for p in ys]
    to_z = [device(x, y, lax.rem(z + k, NZ), c) for k in range(1, NZ)]

    rows = ROWS // STEPS
    loads = []
    for step in range(STEPS):
        at = pl.ds(step * rows, rows)
        for i, (src, dst) in enumerate(((q_hbm, q_in), (g_hbm, g_in))):
            loads.append(pltpu.make_async_copy(src.at[at], dst.at[at], in_sem.at[2 * step + i]))
    for i, (src, dst) in enumerate(((r1_hbm, r1), (r2_hbm, r2), (rg_hbm, rg))):
        loads.append(pltpu.make_async_copy(src, dst, in_sem.at[2 * STEPS + i]))
    for load in loads:
        load.start()

    barrier = pltpu.get_barrier_semaphore()
    peers = [other, *to_x, *to_y, *to_z]
    for peer in peers:
        pl.semaphore_signal(barrier, inc=1, device_id=peer, device_id_type=pl.DeviceIdType.MESH)

    sent = []

    def send(src, dst, sems, k, to):
        copy = pltpu.make_async_remote_copy(src_ref=src, dst_ref=dst, send_sem=sems.at[0, k], recv_sem=sems.at[1, k],
                                            device_id=to, device_id_type=pl.DeviceIdType.MESH)
        copy.start()
        sent.append(copy)
        return copy

    def gram_half(h, at):
        def slab(i):
            return slab_h[i, at], slab_l[i, at]

        q = join([slab(0), slab(3)], 1)
        return mm3(slab(h), q, TN), mm3(slab(2 + h), slab(3 * h), TN)

    for step in range(STEPS):
        at = slice(step * rows, (step + 1) * rows)
        loads[2 * step].wait()
        loads[2 * step + 1].wait()
        for i, (src, s) in enumerate(((q_in, A), (g_in, B), (g_in, A), (q_in, B))):
            slab_h[i, at], slab_l[i, at] = halves(src[at, s])
        wide, block = gram_half(1 - c, at)
        if step:
            wide, block = acc[:, :W] + wide, acc[:, W:] + block
        if step < STEPS - 1:
            acc[:, :W], acc[:, W:] = wide, block

    def put_theirs(i, j, tile, value):
        theirs[i, j, tile] = value

    pack_half(1 - c, wide, block, put_theirs)
    pl.semaphore_wait(barrier, len(peers))
    core = send(theirs, core_in, core_sem, 0, other)
    wide, block = gram_half(c, slice(None))
    core.wait_recv()

    def put_mine(i, j, tile, value):
        mine[i, j, tile] = value + core_in[i, j, tile]

    pack_half(c, wide, block, put_mine)

    def span(part):
        return pl.ds(part[0], part[1])

    def line(ref, part, at):
        return ref.at[at, :, span(part)] if part[2] else ref.at[:, at, span(part)]

    one = [[send(line(mine, part, (xs if part[2] else ys)[k]), one_in[p].at[k], one_sem, 3 * p + k, (to_x if part[2] else to_y)[k])
            for k in range(3)] for p, part in enumerate(PARTS)]

    for load in loads[2 * STEPS :]:
        load.wait()
    small = small_inverses((r1[...], r2[...]))
    for m, out in enumerate((inv1, inv2)):
        out[...] = jnp.zeros((W, W), jnp.float32)
        for b in range(4):
            out[b * 128 : b * 128 + 128, b * 128 : b * 128 + 128] = small[4 * m + b]

    two_copies = []
    for p, part in enumerate(PARTS):
        lo, hi = part[0], part[0] + part[1]
        for copy in one[p]:
            copy.wait_recv()
        here = mine[x, :, lo:hi] if part[2] else mine[:, y, lo:hi]
        two[p][...] = (here + one_in[p][0]) + (one_in[p][1] + one_in[p][2])
        two_copies.append([send(two[p].at[(ys if part[2] else xs)[k]], two_in[p].at[k], two_sem, 3 * p + k, (to_y if part[2] else to_x)[k])
                           for k in range(3)])

    join_inverses((r1, r2), (inv1, inv2))
    for pair, ref in ((inv1_p, inv1), (inv2_p, inv2), (r2_p, r2)):
        pair[0][...], pair[1][...] = halves(ref[...])

    z_copies = []
    for p, part in enumerate(PARTS):
        lo, hi = part[0], part[0] + part[1]
        for copy in two_copies[p]:
            copy.wait_recv()
        own[lo:hi] = (two[p][y if part[2] else x] + two_in[p][0]) + (two_in[p][1] + two_in[p][2])
        z_copies.append([send(own.at[span(part)], z_in.at[k, span(part)], z_sem, 7 * p + k, to_z[k]) for k in range(NZ - 1)])

    def pair_of(refs):
        return refs[0][...], refs[1][...]

    both = halves(mm3(pair_of(inv1_p), pair_of(inv2_p)))
    both_p[0][...], both_p[1][...] = both
    for step in range(STEPS):
        at = slice(step * rows, (step + 1) * rows)
        g0, g1 = (slab_h[2, at], slab_l[2, at]), (slab_h[1, at], slab_l[1, at])
        u_buf[at, A] = mm3(join([g0, g1], 1), cut(both, A), NT)
        u_buf[at, B] = mm3(g1, cut(both, B, B), NT)
    u_copy = pltpu.make_async_copy(u_buf, u_hbm, u_sem)
    u_copy.start()
    r2_v = pair_of(r2_p)
    t = halves(mm3(halves(r1[...]), halves(rg[...]), NT))
    k2[...] = mm3(r2_v, t)
    k1[...] = mm3(t, r2_v)

    four = []
    for p, part in enumerate(PARTS):
        lo, hi = part[0], part[0] + part[1]
        total = own[lo:hi]
        for k, copy in enumerate(z_copies[p]):
            copy.wait_recv()
            total = total + z_in[k, lo:hi]
        whole[c, x, y, lo:hi] = total
        ref = whole.at[c, x, y, span(part)]
        four.append([send(ref, ref, four_sem, 3 * p + k, (to_y if part[2] else to_x)[k]) for k in range(3)])
    five = []
    last = []
    mine_all = whole.at[c]
    for p, part in enumerate(PARTS):
        for copy in four[p]:
            copy.wait_recv()
        ref = line(mine_all, part, x if part[2] else y)
        five.append([send(ref, ref, five_sem, 3 * p + k, (to_x if part[2] else to_y)[k]) for k in range(3)])
        last.append(send(ref, ref, last_sem, 4 * p, other))
    for k in (0, 2, 1):
        for p, part in enumerate(PARTS):
            five[p][k].wait_recv()
            ref = line(mine_all, part, lax.rem((x if part[2] else y) + 3 - k, 4))
            last.append(send(ref, ref, last_sem, 4 * p + 1 + k, other))
    for copy in last:
        copy.wait_recv()

    for group in range(32):
        at = (group // 16, (group // 4) % 4, group % 4)
        for tile in range(8):
            r, l = group * 16 + (tile // 4) * 8, (tile % 4) * 128
            square[r : r + 8, l : l + 128] = whole[(*at, tile)]
        if group % 16 < 2:
            l = group // 16 * HALF + group % 16 * 128
            diag[:, l : l + 128] = whole[(*at, 8)]
    m2_out[A], m2_out[B] = middle(square, diag[0:1], k1, k2, pair_of(r2_p), pair_of(inv1_p), pair_of(inv2_p), pair_of(both_p))
    u_copy.wait()
    for copy in sent:
        copy.wait_send()


def main(q_final, r_first, r_second, q_grad, r_grad):
    hbm = pl.BlockSpec(memory_space=pl.ANY)
    f32, bf16 = jnp.float32, jnp.bfloat16
    tile = (8, 128)
    scratch = [pltpu.VMEM((ROWS, W), f32)] * 2
    scratch += [pltpu.VMEM((4, ROWS, HALF), bf16)] * 2
    scratch += [pltpu.VMEM((W, W), f32)] * 7
    scratch += [pltpu.VMEM((ROWS, W), f32), pltpu.VMEM((W, W), f32), pltpu.VMEM((8, W), f32), pltpu.VMEM((HALF, W + HALF), f32)]
    scratch += [pltpu.VMEM((W, W), bf16)] * 8
    scratch += [pltpu.VMEM((NX, NY, 9, *tile), f32)] * 3
    scratch += [pltpu.VMEM((9, *tile), f32), pltpu.VMEM((NZ - 1, 9, *tile), f32), pltpu.VMEM((2, NX, NY, 9, *tile), f32)]
    scratch += [pltpu.VMEM((3, 4, part[1], *tile), f32) for part in PARTS]
    scratch += [pltpu.VMEM((4, part[1], *tile), f32) for part in PARTS]
    scratch += [pltpu.VMEM((3, part[1], *tile), f32) for part in PARTS]
    n = len(PARTS)
    scratch += [pltpu.SemaphoreType.DMA((2 * STEPS + 3,)), pltpu.SemaphoreType.DMA]
    scratch += [pltpu.SemaphoreType.DMA((2, k)) for k in (1, 3 * n, 3 * n, 7 * n, 3 * n, 3 * n, 4 * n)]
    return pl.pallas_call(
        main_kernel,
        in_specs=[hbm] * 5,
        out_specs=[pl.BlockSpec(memory_space=pltpu.VMEM), hbm],
        out_shape=[jax.ShapeDtypeStruct((W, W), f32), jax.ShapeDtypeStruct((ROWS, W), f32)],
        scratch_shapes=scratch,
        compiler_params=pltpu.CompilerParams(collective_id=0, has_side_effects=True, vmem_limit_bytes=60 << 20),
        name="main",
    )(q_final, r_first, r_second, q_grad, r_grad)


def finish_kernel(u, q, m2, out):
    out[...] = u[...] + mm3(halves(q[...]), halves(m2[...]))


def finish(u, q_final, m2):
    rows = ROWS // 6
    spec = pl.BlockSpec((rows, W), lambda i: (i, 0))
    small = pl.BlockSpec((W, W), lambda i: (0, 0))
    return pl.pallas_call(
        finish_kernel,
        grid=(6,),
        in_specs=[spec, spec, small],
        out_specs=spec,
        out_shape=jax.ShapeDtypeStruct((ROWS, W), jnp.float32),
        compiler_params=pltpu.CompilerParams(vmem_limit_bytes=48 << 20),
        name="finish",
    )(u, q_final, m2)


def local(q_final, r_first, r_second, q_grad, r_grad):
    m2, u = main(q_final, r_first, r_second, q_grad, r_grad)
    return finish(u, q_final, m2)


def solution(mesh):
    placed = (P("rows", None), P(), P(), P("rows", None), P())
    return jax.shard_map(local, mesh=mesh, in_specs=placed, out_specs=P("rows", None), check_vma=False)
```

```python
import jax
import jax.numpy as jnp
from jax import lax
from jax.experimental import pallas as pl
from jax.experimental.pallas import tpu as pltpu
from jax.sharding import PartitionSpec as P

HIGHEST = lax.Precision.HIGHEST
W, HALF = 512, 256
NX, NY, NZ = 4, 4, 8
ROWS, STEPS = 1536, 3
PARTS = ((0, 5, True), (5, 4, False))
FAR_4, FAR_8 = (1, 0, 2), (3, 2, 4, 1, 5, 0, 6)
NN, NT, TN = ((1,), (0,)), ((1,), (1,)), ((0,), (0,))
A, B = slice(0, HALF), slice(HALF, W)


def mm(a, b):
    return lax.dot_general(a, b, (NN, ((), ())), precision=HIGHEST, preferred_element_type=jnp.float32)


def halves(a):
    high = a.astype(jnp.bfloat16)
    return high, (a - high.astype(jnp.float32)).astype(jnp.bfloat16)


def cut(pair, *index):
    return pair[0][index], pair[1][index]


def join(pairs, axis):
    return tuple(jnp.concatenate([p[i] for p in pairs], axis=axis) for i in range(2))


def mm3(a, b, dims=NN):
    (ah, al), (bh, bl) = a, b

    def dot(u, v):
        return lax.dot_general(u, v, (dims, ((), ())), preferred_element_type=jnp.float32)

    return dot(ah, bh) + (dot(ah, bl) + dot(al, bh))


def iotas(rows, cols):
    return lax.broadcasted_iota(jnp.int32, (rows, cols), 0), lax.broadcasted_iota(jnp.int32, (rows, cols), 1)


def small_inverses(uppers, size=128):
    row, col = iotas(size, size)
    eye, above = row == col, col > row
    block = [u[b : b + size, b : b + size] for u in uppers for b in range(0, W, size)]
    inv = []
    for u in block:
        d_row = 1.0 / jnp.sum(jnp.where(eye, u, 0.0), axis=0, keepdims=True)
        d_col = 1.0 / jnp.sum(jnp.where(eye, u, 0.0), axis=1, keepdims=True)
        pair = above & (row // 2 == col // 2)
        inv.append(jnp.where(eye, d_row, jnp.where(pair, -(u * d_col) * d_row, 0.0)))
    s = 2
    while s < size:
        between = above & (row // (2 * s) == col // (2 * s)) & (row // s != col // s)
        half = [mm(jnp.where(between, u, 0.0), x) for u, x in zip(block, inv)]
        inv = [x - mm(x, h) for x, h in zip(inv, half)]
        s *= 2
    return inv


def join_inverses(uppers, outs, size=128):
    s = size
    while s < W:
        for u, out in zip(uppers, outs):
            for b in range(0, W, 2 * s):
                top, low = slice(b, b + s), slice(b + s, b + 2 * s)
                out[top, low] = -mm(out[top, top], mm(u[top, low], out[low, low]))
        s *= 2


def place():
    me = lax.axis_index("rows")
    c = lax.rem(me, 2)
    z = lax.rem(lax.div(me, 2), NZ)
    y = lax.rem(lax.div(me, 2 * NZ), NY)
    x = lax.div(me, 2 * NZ * NY)
    return x, y, z, c


def device(x, y, z, c):
    return (((x * NY + y) * NZ + z) * 2 + c,)


def pack_half(h, wide, square, put):
    row, col = iotas(HALF, HALF)
    low, eye = row >= col, row == col
    is_top = jnp.full((HALF, HALF), h, jnp.int32) == 0
    parts = (jnp.where(low & is_top, square, wide[:, A]), jnp.where(low | is_top, wide[:, B], square))
    diag = jnp.sum(jnp.where(eye, jnp.where(is_top, wide[:, A], square), 0.0), axis=0, keepdims=True)
    first = lax.broadcasted_iota(jnp.int32, (8, 128), 0) == 0
    for group in range(16):
        for tile in range(8):
            r, l = group * 16 + (tile // 4) * 8, (tile % 4) * 128
            put(group // 4, group % 4, tile, parts[l // HALF][r : r + 8, l % HALF : l % HALF + 128])
        extra = jnp.zeros((8, 128), jnp.float32)
        if group < 2:
            extra = jnp.where(first, jnp.broadcast_to(diag[:, group * 128 : group * 128 + 128], (8, 128)), 0.0)
        put(group // 4, group % 4, 8, extra)


def copy_lower(m, low, strict):
    return jnp.where(low, m, 0.0) + jnp.where(strict, m, 0.0).T


def symmetric(b00, b10, b11):
    row, col = iotas(HALF, HALF)
    low, strict = row >= col, row > col
    top = jnp.concatenate([copy_lower(b00, low, strict), b10.T], axis=1)
    return jnp.concatenate([top, jnp.concatenate([b10, copy_lower(b11, low, strict)], axis=1)], axis=0)


def middle(square, diag, k1, k2, r2, inv1, inv2, both):
    row, col = iotas(HALF, HALF)
    low, strict, above, eye = row >= col, row > col, row < col, row == col
    second = halves(symmetric(*(k2[i, j] - square[i, j] for i, j in ((A, A), (B, A), (B, B)))))
    grams = []
    for s in (A, B):
        upper = jnp.where(above, square[s, s], 0.0)
        grams.append(upper + upper.T + jnp.where(eye, jnp.broadcast_to(diag[:, s], (HALF, HALF)), 0.0))
    g01 = square[A, B]
    gram_a = halves(jnp.concatenate([grams[0], g01.T], axis=0))
    gram_b = halves(jnp.concatenate([g01, grams[1]], axis=0))
    cross_a = jnp.concatenate([jnp.where(low, square[A, A], 0.0), square[B, A]], axis=0)
    y_a = halves(cross_a + mm3(second, gram_a))
    y_bb = halves(jnp.where(low, square[B, B], 0.0) + mm3(cut(second, B), gram_b))
    w_a = halves(mm3(y_a, cut(r2, A, A)))
    w_bb = halves(mm3(join([cut(y_a, B), y_bb], 1), cut(r2, slice(None), B)))
    z_aa = mm3(cut(inv2, A), w_a)
    z_b = mm3(cut(inv2, B, B), join([cut(w_a, B), w_bb], 1))
    first = halves(symmetric(k1[A, A] - z_aa, k1[B, A] - z_b[:, A], k1[B, B] - z_b[:, B]))
    v = halves(times_lower(first, inv1))
    add = times_lower(second, both)
    return add[A] + mm3(cut(r2, A), v), add[B] + mm3(cut(r2, B, B), cut(v, B))


def times_lower(a, upper):
    return jnp.concatenate([mm3(a, cut(upper, A), NT), mm3(cut(a, slice(None), B), cut(upper, B, B), NT)], axis=1)


def main_kernel(q_hbm, r1_hbm, r2_hbm, g_hbm, rg_hbm, u_buf, slab_h, slab_l, m2_h, m2_l, *scratch):
    scratch = list(scratch)
    q_in, g_in, r1, r2, rg, inv1, inv2, k1, k2, square, diag, acc = (scratch.pop(0) for _ in range(12))
    bf = [scratch.pop(0) for _ in range(8)]
    r2_p, inv1_p, inv2_p, both_p = (tuple(bf[i : i + 2]) for i in range(0, 8, 2))
    theirs, core_in, mine, own, z_in, whole = (scratch.pop(0) for _ in range(6))
    one_in, two, two_in = ([scratch.pop(0) for _ in PARTS] for _ in range(3))
    in_sem, core_sem, one_sem, two_sem, z_sem, four_sem, five_sem, last_sem = (scratch.pop(0) for _ in range(8))
    x, y, z, c = place()
    other = device(x, y, z, 1 - c)
    xs = [lax.rem(x + k, NX) for k in range(1, NX)]
    ys = [lax.rem(y + k, NY) for k in range(1, NY)]
    to_x = [device(p, y, z, c) for p in xs]
    to_y = [device(x, p, z, c) for p in ys]
    to_z = [device(x, y, lax.rem(z + k, NZ), c) for k in range(1, NZ)]

    rows = ROWS // STEPS
    loads = []
    for step in range(STEPS):
        at = pl.ds(step * rows, rows)
        for i, (src, dst) in enumerate(((q_hbm, q_in), (g_hbm, g_in))):
            loads.append(pltpu.make_async_copy(src.at[at], dst.at[at], in_sem.at[2 * step + i]))
    for i, (src, dst) in enumerate(((r1_hbm, r1), (r2_hbm, r2), (rg_hbm, rg))):
        loads.append(pltpu.make_async_copy(src, dst, in_sem.at[2 * STEPS + i]))
    for load in loads:
        load.start()

    barrier = pltpu.get_barrier_semaphore()
    peers = [other, *to_x, *to_y, *to_z]
    for peer in peers:
        pl.semaphore_signal(barrier, inc=1, device_id=peer, device_id_type=pl.DeviceIdType.MESH)

    def pair_of(refs):
        return refs[0][...], refs[1][...]

    sent = []

    def send(src, dst, sems, k, to):
        copy = pltpu.make_async_remote_copy(src_ref=src, dst_ref=dst, send_sem=sems.at[0, k], recv_sem=sems.at[1, k],
                                            device_id=to, device_id_type=pl.DeviceIdType.MESH)
        copy.start()
        sent.append(copy)
        return copy

    def gram_half(h, at):
        def slab(i):
            return slab_h[i, at], slab_l[i, at]

        q = join([slab(0), slab(3)], 1)
        return mm3(slab(h), q, TN), mm3(slab(2 + h), slab(3 * h), TN)

    for step in range(STEPS):
        at = slice(step * rows, (step + 1) * rows)
        loads[2 * step].wait()
        loads[2 * step + 1].wait()
        for i, (src, s) in enumerate(((q_in, A), (g_in, B), (g_in, A), (q_in, B))):
            slab_h[i, at], slab_l[i, at] = halves(src[at, s])
        wide, block = gram_half(1 - c, at)
        if step:
            wide, block = acc[:, :W] + wide, acc[:, W:] + block
        if step < STEPS - 1:
            acc[:, :W], acc[:, W:] = wide, block

    def put_theirs(i, j, tile, value):
        theirs[i, j, tile] = value

    pack_half(1 - c, wide, block, put_theirs)
    pl.semaphore_wait(barrier, len(peers))
    core = send(theirs, core_in, core_sem, 0, other)
    wide, block = gram_half(c, slice(None))
    core.wait_recv()

    def put_mine(i, j, tile, value):
        mine[i, j, tile] = value + core_in[i, j, tile]

    pack_half(c, wide, block, put_mine)

    def span(part):
        return pl.ds(part[0], part[1])

    def line(ref, part, at):
        return ref.at[at, :, span(part)] if part[2] else ref.at[:, at, span(part)]

    one = [[send(line(mine, part, (xs if part[2] else ys)[k]), one_in[p].at[k], one_sem, 3 * p + k, (to_x if part[2] else to_y)[k])
            for k in FAR_4] for p, part in enumerate(PARTS)]

    for load in loads[2 * STEPS :]:
        load.wait()
    r2_p[0][...], r2_p[1][...] = halves(r2[...])

    two_copies = []
    for p, part in enumerate(PARTS):
        lo, hi = part[0], part[0] + part[1]
        for copy in one[p]:
            copy.wait_recv()
        here = mine[x, :, lo:hi] if part[2] else mine[:, y, lo:hi]
        two[p][...] = (here + one_in[p][0]) + (one_in[p][1] + one_in[p][2])
        two_copies.append([send(two[p].at[(ys if part[2] else xs)[k]], two_in[p].at[k], two_sem, 3 * p + k, (to_y if part[2] else to_x)[k])
                           for k in FAR_4])

    r2_v = pair_of(r2_p)
    r1_v, rg_v = halves(r1[...]), halves(rg[...])
    t = halves(jnp.concatenate([mm3(cut(r1_v, A), rg_v, NT), mm3(cut(r1_v, B, B), cut(rg_v, slice(None), B), NT)], axis=0))
    k2[A, A], k2[B] = mm3(cut(r2_v, A), cut(t, slice(None), A)), mm3(cut(r2_v, B, B), cut(t, B))
    k1[:, A], k1[B, B] = mm3(cut(t, slice(None), A), cut(r2_v, A, A)), mm3(cut(t, B), cut(r2_v, slice(None), B))

    z_copies = []
    for p, part in enumerate(PARTS):
        lo, hi = part[0], part[0] + part[1]
        for copy in two_copies[p]:
            copy.wait_recv()
        own[lo:hi] = (two[p][y if part[2] else x] + two_in[p][0]) + (two_in[p][1] + two_in[p][2])
        z_copies.append([send(own.at[span(part)], z_in.at[k, span(part)], z_sem, 7 * p + k, to_z[k]) for k in FAR_8])

    small = small_inverses((r1[...], r2[...]))
    for m, out in enumerate((inv1, inv2)):
        out[...] = jnp.zeros((W, W), jnp.float32)
        for b in range(4):
            out[b * 128 : b * 128 + 128, b * 128 : b * 128 + 128] = small[4 * m + b]

    join_inverses((r1, r2), (inv1, inv2))
    for pair, ref in ((inv1_p, inv1), (inv2_p, inv2)):
        pair[0][...], pair[1][...] = halves(ref[...])

    i1, i2 = pair_of(inv1_p), pair_of(inv2_p)
    for i, j in ((A, A), (A, B), (B, B)):
        inner = slice(i.start, j.stop)
        both_p[0][i, j], both_p[1][i, j] = halves(mm3(cut(i1, i, inner), cut(i2, inner, j)))
    both_p[0][B, A], both_p[1][B, A] = jnp.zeros((HALF, HALF), jnp.bfloat16), jnp.zeros((HALF, HALF), jnp.bfloat16)
    both = pair_of(both_p)

    four = []
    for p, part in enumerate(PARTS):
        lo, hi = part[0], part[0] + part[1]
        for copy in z_copies[p]:
            copy.wait_recv()
        total = own[lo:hi]
        for k in range(NZ - 1):
            total = total + z_in[k, lo:hi]
        whole[c, x, y, lo:hi] = total
        ref = whole.at[c, x, y, span(part)]
        four.append([send(ref, ref, four_sem, 3 * p + k, (to_y if part[2] else to_x)[k]) for k in FAR_4])
    for step in range(STEPS):
        at = slice(step * rows, (step + 1) * rows)
        g0, g1 = (slab_h[2, at], slab_l[2, at]), (slab_h[1, at], slab_l[1, at])
        u_buf[at, A] = mm3(join([g0, g1], 1), cut(both, A), NT)
        u_buf[at, B] = mm3(g1, cut(both, B, B), NT)

    five = []
    last = []
    mine_all = whole.at[c]
    for p, part in enumerate(PARTS):
        for copy in four[p]:
            copy.wait_recv()
        ref = line(mine_all, part, x if part[2] else y)
        five.append([send(ref, ref, five_sem, 3 * p + k, (to_x if part[2] else to_y)[k]) for k in FAR_4])
        last.append(send(ref, ref, last_sem, 4 * p, other))
    for k in (0, 2, 1):
        for p, part in enumerate(PARTS):
            five[p][FAR_4.index(k)].wait_recv()
            ref = line(mine_all, part, lax.rem((x if part[2] else y) + 3 - k, 4))
            last.append(send(ref, ref, last_sem, 4 * p + 1 + k, other))
    for copy in last:
        copy.wait_recv()

    for group in range(32):
        at = (group // 16, (group // 4) % 4, group % 4)
        for tile in range(8):
            r, l = group * 16 + (tile // 4) * 8, (tile % 4) * 128
            square[r : r + 8, l : l + 128] = whole[(*at, tile)]
        if group % 16 < 2:
            l = group // 16 * HALF + group % 16 * 128
            diag[:, l : l + 128] = whole[(*at, 8)]
    for s, m in zip((A, B), middle(square, diag[0:1], k1, k2, pair_of(r2_p), pair_of(inv1_p), pair_of(inv2_p), pair_of(both_p))):
        m2_h[s], m2_l[s] = halves(m)
    for copy in sent:
        copy.wait_send()


def main(q_final, r_first, r_second, q_grad, r_grad):
    hbm = pl.BlockSpec(memory_space=pl.ANY)
    f32, bf16 = jnp.float32, jnp.bfloat16
    tile = (8, 128)
    scratch = [pltpu.VMEM((ROWS, W), f32)] * 2
    scratch += [pltpu.VMEM((W, W), f32)] * 7
    scratch += [pltpu.VMEM((W, W), f32), pltpu.VMEM((8, W), f32), pltpu.VMEM((HALF, W + HALF), f32)]
    scratch += [pltpu.VMEM((W, W), bf16)] * 8
    scratch += [pltpu.VMEM((NX, NY, 9, *tile), f32)] * 3
    scratch += [pltpu.VMEM((9, *tile), f32), pltpu.VMEM((NZ - 1, 9, *tile), f32), pltpu.VMEM((2, NX, NY, 9, *tile), f32)]
    scratch += [pltpu.VMEM((3, 4, part[1], *tile), f32) for part in PARTS]
    scratch += [pltpu.VMEM((4, part[1], *tile), f32) for part in PARTS]
    scratch += [pltpu.VMEM((3, part[1], *tile), f32) for part in PARTS]
    n = len(PARTS)
    scratch += [pltpu.SemaphoreType.DMA((2 * STEPS + 3,))]
    scratch += [pltpu.SemaphoreType.DMA((2, k)) for k in (1, 3 * n, 3 * n, 7 * n, 3 * n, 3 * n, 4 * n)]
    return pl.pallas_call(
        main_kernel,
        in_specs=[hbm] * 5,
        out_specs=[pl.BlockSpec(memory_space=pltpu.VMEM)] * 5,
        out_shape=[pltpu.VMEM((ROWS, W), f32)] + [pltpu.VMEM((4, ROWS, HALF), bf16)] * 2 + [pltpu.VMEM((W, W), bf16)] * 2,
        scratch_shapes=scratch,
        compiler_params=pltpu.CompilerParams(collective_id=0, has_side_effects=True, vmem_limit_bytes=48 << 20),
        name="main",
    )(q_final, r_first, r_second, q_grad, r_grad)


def finish_kernel(u, slab_h, slab_l, m2_h, m2_l, out_hbm, out, sem):
    m2 = m2_h[...], m2_l[...]
    stores = []
    for step in range(6):
        at = slice(step * 256, (step + 1) * 256)
        q = join([(slab_h[i, at], slab_l[i, at]) for i in (0, 3)], 1)
        out[at] = u[at] + mm3(q, m2)
        stores.append(pltpu.make_async_copy(out.at[at], out_hbm.at[at], sem.at[step]))
        stores[-1].start()
    for store in stores:
        store.wait()


def finish(*operands):
    return pl.pallas_call(
        finish_kernel,
        in_specs=[pl.BlockSpec(memory_space=pltpu.VMEM)] * 5,
        out_specs=pl.BlockSpec(memory_space=pl.ANY),
        out_shape=jax.ShapeDtypeStruct((ROWS, W), jnp.float32),
        scratch_shapes=[pltpu.VMEM((ROWS, W), jnp.float32), pltpu.SemaphoreType.DMA((6,))],
        compiler_params=pltpu.CompilerParams(vmem_limit_bytes=12 << 20),
        name="finish",
    )(*operands)


def local(q_final, r_first, r_second, q_grad, r_grad):
    return finish(*main(q_final, r_first, r_second, q_grad, r_grad))


def solution(mesh):
    placed = (P("rows", None), P(), P(), P("rows", None), P())
    return jax.shard_map(local, mesh=mesh, in_specs=placed, out_specs=P("rows", None), check_vma=False)
```

```python
import jax
import jax.numpy as jnp
from jax import lax
from jax.experimental import pallas as pl
from jax.experimental.pallas import tpu as pltpu
from jax.sharding import PartitionSpec as P

HIGHEST = lax.Precision.HIGHEST
W, HALF = 512, 256
NX, NY, NZ = 4, 4, 8
ROWS, STEPS = 1536, 3
PARTS = ((0, 4, True), (4, 4, False))
SLOTS = ((0, 5), (5, 9))
FAR_4, FAR_8 = (1, 0, 2), (3, 2, 4, 1, 5, 0, 6)
NN, NT, TN = ((1,), (0,)), ((1,), (1,)), ((0,), (0,))
A, B = slice(0, HALF), slice(HALF, W)


def mm(a, b):
    return lax.dot_general(a, b, (NN, ((), ())), precision=HIGHEST, preferred_element_type=jnp.float32)


def halves(a):
    high = a.astype(jnp.bfloat16)
    return high, (a - high.astype(jnp.float32)).astype(jnp.bfloat16)


def cut(pair, *index):
    return pair[0][index], pair[1][index]


def join(pairs, axis):
    return tuple(jnp.concatenate([p[i] for p in pairs], axis=axis) for i in range(2))


def mm3(a, b, dims=NN):
    (ah, al), (bh, bl) = a, b

    def dot(u, v):
        return lax.dot_general(u, v, (dims, ((), ())), preferred_element_type=jnp.float32)

    return dot(ah, bh) + (dot(ah, bl) + dot(al, bh))


def iotas(rows, cols):
    return lax.broadcasted_iota(jnp.int32, (rows, cols), 0), lax.broadcasted_iota(jnp.int32, (rows, cols), 1)


def small_inverses(uppers, size=128):
    row, col = iotas(size, size)
    eye, above = row == col, col > row
    block = [u[b : b + size, b : b + size] for u in uppers for b in range(0, W, size)]
    inv = []
    for u in block:
        d_row = 1.0 / jnp.sum(jnp.where(eye, u, 0.0), axis=0, keepdims=True)
        d_col = 1.0 / jnp.sum(jnp.where(eye, u, 0.0), axis=1, keepdims=True)
        pair = above & (row // 2 == col // 2)
        inv.append(jnp.where(eye, d_row, jnp.where(pair, -(u * d_col) * d_row, 0.0)))
    s = 2
    while s < size:
        between = above & (row // (2 * s) == col // (2 * s)) & (row // s != col // s)
        half = [mm(jnp.where(between, u, 0.0), x) for u, x in zip(block, inv)]
        inv = [x - mm(x, h) for x, h in zip(inv, half)]
        s *= 2
    return inv


def join_inverses(uppers, outs, size=128):
    s = size
    while s < W:
        for u, out in zip(uppers, outs):
            for b in range(0, W, 2 * s):
                top, low = slice(b, b + s), slice(b + s, b + 2 * s)
                out[top, low] = -mm(out[top, top], mm(u[top, low], out[low, low]))
        s *= 2


def place():
    me = lax.axis_index("rows")
    c = lax.rem(me, 2)
    z = lax.rem(lax.div(me, 2), NZ)
    y = lax.rem(lax.div(me, 2 * NZ), NY)
    x = lax.div(me, 2 * NZ * NY)
    return x, y, z, c


def device(x, y, z, c):
    return (((x * NY + y) * NZ + z) * 2 + c,)


def pack_half(h, wide, square, put):
    row, col = iotas(HALF, HALF)
    low, eye = row >= col, row == col
    is_top = jnp.full((HALF, HALF), h, jnp.int32) == 0
    parts = (jnp.where(low & is_top, square, wide[:, A]), jnp.where(low | is_top, wide[:, B], square))
    diag = jnp.sum(jnp.where(eye, jnp.where(is_top, wide[:, A], square), 0.0), axis=0, keepdims=True)
    first = lax.broadcasted_iota(jnp.int32, (8, 128), 0)
    for group in range(16):
        for tile in range(8):
            r, l = group * 16 + (tile // 4) * 8, (tile % 4) * 128
            put(group // 4, group % 4, tile, parts[l // HALF][r : r + 8, l % HALF : l % HALF + 128])
        extra = jnp.zeros((8, 128), jnp.float32)
        if group == 0:
            lines = [jnp.broadcast_to(diag[:, i * 128 : i * 128 + 128], (8, 128)) for i in range(2)]
            extra = jnp.where(first == 0, lines[0], jnp.where(first == 1, lines[1], 0.0))
        put(group // 4, group % 4, 8, extra)


def copy_lower(m, low, strict):
    return jnp.where(low, m, 0.0) + jnp.where(strict, m, 0.0).T


def symmetric(b00, b10, b11):
    row, col = iotas(HALF, HALF)
    low, strict = row >= col, row > col
    top = jnp.concatenate([copy_lower(b00, low, strict), b10.T], axis=1)
    return jnp.concatenate([top, jnp.concatenate([b10, copy_lower(b11, low, strict)], axis=1)], axis=0)


def middle(square, diag, k1, k2, r2, inv1, inv2, both):
    row, col = iotas(HALF, HALF)
    low, strict, above, eye = row >= col, row > col, row < col, row == col
    second = halves(symmetric(*(k2[i, j] - square[i, j] for i, j in ((A, A), (B, A), (B, B)))))
    grams = []
    for s in (A, B):
        upper = jnp.where(above, square[s, s], 0.0)
        grams.append(upper + upper.T + jnp.where(eye, jnp.broadcast_to(diag[:, s], (HALF, HALF)), 0.0))
    g01 = square[A, B]
    gram_a = halves(jnp.concatenate([grams[0], g01.T], axis=0))
    gram_b = halves(jnp.concatenate([g01, grams[1]], axis=0))
    cross_a = jnp.concatenate([jnp.where(low, square[A, A], 0.0), square[B, A]], axis=0)
    y_a = halves(cross_a + mm3(second, gram_a))
    y_bb = halves(jnp.where(low, square[B, B], 0.0) + mm3(cut(second, B), gram_b))
    w_a = halves(mm3(y_a, cut(r2, A, A)))
    w_bb = halves(mm3(join([cut(y_a, B), y_bb], 1), cut(r2, slice(None), B)))
    z_aa = mm3(cut(inv2, A), w_a)
    z_b = mm3(cut(inv2, B, B), join([cut(w_a, B), w_bb], 1))
    first = halves(symmetric(k1[A, A] - z_aa, k1[B, A] - z_b[:, A], k1[B, B] - z_b[:, B]))
    v = halves(times_lower(first, inv1))
    add = times_lower(second, both)
    return add[A] + mm3(cut(r2, A), v), add[B] + mm3(cut(r2, B, B), cut(v, B))


def times_lower(a, upper):
    return jnp.concatenate([mm3(a, cut(upper, A), NT), mm3(cut(a, slice(None), B), cut(upper, B, B), NT)], axis=1)


def main_kernel(q_hbm, r1_hbm, r2_hbm, g_hbm, rg_hbm, u_buf, slab_h, slab_l, m2_h, m2_l, *scratch):
    scratch = list(scratch)
    q_in, g_in, r1, r2, rg, inv1, inv2, k1, k2, square, diag, acc = (scratch.pop(0) for _ in range(12))
    bf = [scratch.pop(0) for _ in range(8)]
    r2_p, inv1_p, inv2_p, both_p = (tuple(bf[i : i + 2]) for i in range(0, 8, 2))
    theirs, core_in, mine, own, z_in, whole = (scratch.pop(0) for _ in range(6))
    one_in, two, two_in = ([scratch.pop(0) for _ in PARTS] for _ in range(3))
    e_in, lines = scratch.pop(0), scratch.pop(0)
    in_sem, core_sem, one_sem, two_sem, z_sem, four_sem, five_sem, last_sem, e_sem = (scratch.pop(0) for _ in range(9))
    x, y, z, c = place()
    other = device(x, y, z, 1 - c)
    xs = [lax.rem(x + k, NX) for k in range(1, NX)]
    ys = [lax.rem(y + k, NY) for k in range(1, NY)]
    to_x = [device(p, y, z, c) for p in xs]
    to_y = [device(x, p, z, c) for p in ys]
    to_z = [device(x, y, lax.rem(z + k, NZ), c) for k in range(1, NZ)]

    rows = ROWS // STEPS
    loads = []
    for step in range(STEPS):
        at = pl.ds(step * rows, rows)
        for i, (src, dst) in enumerate(((q_hbm, q_in), (g_hbm, g_in))):
            loads.append(pltpu.make_async_copy(src.at[at], dst.at[at], in_sem.at[2 * step + i]))
    for i, (src, dst) in enumerate(((r1_hbm, r1), (r2_hbm, r2), (rg_hbm, rg))):
        loads.append(pltpu.make_async_copy(src, dst, in_sem.at[2 * STEPS + i]))
    for load in loads:
        load.start()

    barrier = pltpu.get_barrier_semaphore()
    peers = [other, *to_x, *to_y, *to_z]
    for peer in peers:
        pl.semaphore_signal(barrier, inc=1, device_id=peer, device_id_type=pl.DeviceIdType.MESH)

    def pair_of(refs):
        return refs[0][...], refs[1][...]

    sent = []

    def send(src, dst, sems, k, to):
        copy = pltpu.make_async_remote_copy(src_ref=src, dst_ref=dst, send_sem=sems.at[0, k], recv_sem=sems.at[1, k],
                                            device_id=to, device_id_type=pl.DeviceIdType.MESH)
        copy.start()
        sent.append(copy)
        return copy

    def gram_half(h, at):
        def slab(i):
            return slab_h[i, at], slab_l[i, at]

        q = join([slab(0), slab(3)], 1)
        return mm3(slab(h), q, TN), mm3(slab(2 + h), slab(3 * h), TN)

    for step in range(STEPS):
        at = slice(step * rows, (step + 1) * rows)
        loads[2 * step].wait()
        loads[2 * step + 1].wait()
        for i, (src, s) in enumerate(((q_in, A), (g_in, B), (g_in, A), (q_in, B))):
            slab_h[i, at], slab_l[i, at] = halves(src[at, s])
        wide, block = gram_half(1 - c, at)
        if step:
            wide, block = acc[:, :W] + wide, acc[:, W:] + block
        if step < STEPS - 1:
            acc[:, :W], acc[:, W:] = wide, block

    def put_theirs(i, j, tile, value):
        theirs[i, j, tile] = value

    pack_half(1 - c, wide, block, put_theirs)
    pl.semaphore_wait(barrier, len(peers))
    core = send(theirs, core_in, core_sem, 0, other)
    wide, block = gram_half(c, slice(None))
    core.wait_recv()

    def put_mine(i, j, tile, value):
        mine[i, j, tile] = value + core_in[i, j, tile]

    pack_half(c, wide, block, put_mine)

    def span(part):
        return pl.ds(part[0], part[1])

    def line(ref, part, at):
        return ref.at[at, :, span(part)] if part[2] else ref.at[:, at, span(part)]

    e_copies = [send(mine.at[0, 0, 8], e_in.at[k], e_sem, k, to_x[k]) for k in FAR_4]
    one = [[send(line(mine, part, (xs if part[2] else ys)[k]), one_in[p].at[k], one_sem, 3 * p + k, (to_x if part[2] else to_y)[k])
            for k in FAR_4] for p, part in enumerate(PARTS)]

    for load in loads[2 * STEPS :]:
        load.wait()
    r2_p[0][...], r2_p[1][...] = halves(r2[...])

    two_copies = []
    for p, part in enumerate(PARTS):
        lo, hi = part[0], part[0] + part[1]
        for copy in one[p]:
            copy.wait_recv()
        here = mine[x, :, lo:hi] if part[2] else mine[:, y, lo:hi]
        two[p][:, 0 : part[1]] = (here + one_in[p][0]) + (one_in[p][1] + one_in[p][2])
        if p == 0:
            for copy in e_copies:
                copy.wait_recv()
            line_sum = (mine[0, 0, 8] + e_in[0]) + (e_in[1] + e_in[2])
            two[p][:, 4] = jnp.broadcast_to(line_sum[None], (4, 8, 128))
        two_copies.append([send(two[p].at[(ys if part[2] else xs)[k]], two_in[p].at[k], two_sem, 3 * p + k, (to_y if part[2] else to_x)[k])
                           for k in FAR_4])

    r2_v = pair_of(r2_p)
    r1_v, rg_v = halves(r1[...]), halves(rg[...])
    t = halves(jnp.concatenate([mm3(cut(r1_v, A), rg_v, NT), mm3(cut(r1_v, B, B), cut(rg_v, slice(None), B), NT)], axis=0))
    k2[A, A], k2[B] = mm3(cut(r2_v, A), cut(t, slice(None), A)), mm3(cut(r2_v, B, B), cut(t, B))
    k1[:, A], k1[B, B] = mm3(cut(t, slice(None), A), cut(r2_v, A, A)), mm3(cut(t, B), cut(r2_v, slice(None), B))

    z_copies = []
    for p, part in enumerate(PARTS):
        lo, hi = SLOTS[p]
        for copy in two_copies[p]:
            copy.wait_recv()
        own[lo:hi] = (two[p][y if part[2] else x] + two_in[p][0]) + (two_in[p][1] + two_in[p][2])
        z_copies.append([send(own.at[pl.ds(lo, hi - lo)], z_in.at[k, pl.ds(lo, hi - lo)], z_sem, 7 * p + k, to_z[k]) for k in FAR_8])

    small = small_inverses((r1[...], r2[...]))
    for m, out in enumerate((inv1, inv2)):
        out[...] = jnp.zeros((W, W), jnp.float32)
        for b in range(4):
            out[b * 128 : b * 128 + 128, b * 128 : b * 128 + 128] = small[4 * m + b]

    join_inverses((r1, r2), (inv1, inv2))
    for pair, ref in ((inv1_p, inv1), (inv2_p, inv2)):
        pair[0][...], pair[1][...] = halves(ref[...])

    i1, i2 = pair_of(inv1_p), pair_of(inv2_p)
    for i, j in ((A, A), (A, B), (B, B)):
        inner = slice(i.start, j.stop)
        both_p[0][i, j], both_p[1][i, j] = halves(mm3(cut(i1, i, inner), cut(i2, inner, j)))
    both_p[0][B, A], both_p[1][B, A] = jnp.zeros((HALF, HALF), jnp.bfloat16), jnp.zeros((HALF, HALF), jnp.bfloat16)
    both = pair_of(both_p)

    four = []
    for p, part in enumerate(PARTS):
        lo, hi = SLOTS[p]
        for copy in z_copies[p]:
            copy.wait_recv()
        total = own[lo:hi]
        for k in range(NZ - 1):
            total = total + z_in[k, lo:hi]
        whole[c, x, y, part[0] : part[0] + part[1]] = total[0 : part[1]]
        if p == 0:
            lines[c] = total[4]
        ref = whole.at[c, x, y, span(part)]
        four.append([send(ref, ref, four_sem, 3 * p + k, (to_y if part[2] else to_x)[k]) for k in FAR_4])
    for step in range(STEPS):
        at = slice(step * rows, (step + 1) * rows)
        g0, g1 = (slab_h[2, at], slab_l[2, at]), (slab_h[1, at], slab_l[1, at])
        u_buf[at, A] = mm3(join([g0, g1], 1), cut(both, A), NT)
        u_buf[at, B] = mm3(g1, cut(both, B, B), NT)

    five = []
    last = [send(lines.at[c], lines.at[c], e_sem, 3, other)]
    mine_all = whole.at[c]
    for p, part in enumerate(PARTS):
        for copy in four[p]:
            copy.wait_recv()
        ref = line(mine_all, part, x if part[2] else y)
        five.append([send(ref, ref, five_sem, 3 * p + k, (to_x if part[2] else to_y)[k]) for k in FAR_4])
        last.append(send(ref, ref, last_sem, 4 * p, other))
    for k in (0, 2, 1):
        for p, part in enumerate(PARTS):
            five[p][FAR_4.index(k)].wait_recv()
            ref = line(mine_all, part, lax.rem((x if part[2] else y) + 3 - k, 4))
            last.append(send(ref, ref, last_sem, 4 * p + 1 + k, other))
    for copy in last:
        copy.wait_recv()

    for group in range(32):
        at = (group // 16, (group // 4) % 4, group % 4)
        for tile in range(8):
            r, l = group * 16 + (tile // 4) * 8, (tile % 4) * 128
            square[r : r + 8, l : l + 128] = whole[(*at, tile)]
    for i in range(4):
        diag[0:1, i * 128 : i * 128 + 128] = lines[i // 2, i % 2 : i % 2 + 1]
    for s, m in zip((A, B), middle(square, diag[0:1], k1, k2, pair_of(r2_p), pair_of(inv1_p), pair_of(inv2_p), pair_of(both_p))):
        m2_h[s], m2_l[s] = halves(m)
    for copy in sent:
        copy.wait_send()


def main(q_final, r_first, r_second, q_grad, r_grad):
    hbm = pl.BlockSpec(memory_space=pl.ANY)
    f32, bf16 = jnp.float32, jnp.bfloat16
    tile = (8, 128)
    scratch = [pltpu.VMEM((ROWS, W), f32)] * 2
    scratch += [pltpu.VMEM((W, W), f32)] * 7
    scratch += [pltpu.VMEM((W, W), f32), pltpu.VMEM((8, W), f32), pltpu.VMEM((HALF, W + HALF), f32)]
    scratch += [pltpu.VMEM((W, W), bf16)] * 8
    scratch += [pltpu.VMEM((NX, NY, 9, *tile), f32)] * 3
    scratch += [pltpu.VMEM((9, *tile), f32), pltpu.VMEM((NZ - 1, 9, *tile), f32), pltpu.VMEM((2, NX, NY, 9, *tile), f32)]
    scratch += [pltpu.VMEM((3, 4, part[1], *tile), f32) for part in PARTS]
    scratch += [pltpu.VMEM((4, hi - lo, *tile), f32) for lo, hi in SLOTS]
    scratch += [pltpu.VMEM((3, hi - lo, *tile), f32) for lo, hi in SLOTS]
    scratch += [pltpu.VMEM((3, *tile), f32), pltpu.VMEM((2, *tile), f32)]
    n = len(PARTS)
    scratch += [pltpu.SemaphoreType.DMA((2 * STEPS + 3,))]
    scratch += [pltpu.SemaphoreType.DMA((2, k)) for k in (1, 3 * n, 3 * n, 7 * n, 3 * n, 3 * n, 4 * n, 4)]
    return pl.pallas_call(
        main_kernel,
        in_specs=[hbm] * 5,
        out_specs=[pl.BlockSpec(memory_space=pltpu.VMEM)] * 5,
        out_shape=[pltpu.VMEM((ROWS, W), f32)] + [pltpu.VMEM((4, ROWS, HALF), bf16)] * 2 + [pltpu.VMEM((W, W), bf16)] * 2,
        scratch_shapes=scratch,
        compiler_params=pltpu.CompilerParams(collective_id=0, has_side_effects=True, vmem_limit_bytes=48 << 20),
        name="main",
    )(q_final, r_first, r_second, q_grad, r_grad)


def finish_kernel(u, slab_h, slab_l, m2_h, m2_l, out_hbm, out, sem):
    m2 = m2_h[...], m2_l[...]
    stores = []
    for step in range(6):
        at = slice(step * 256, (step + 1) * 256)
        q = join([(slab_h[i, at], slab_l[i, at]) for i in (0, 3)], 1)
        out[at] = u[at] + mm3(q, m2)
        stores.append(pltpu.make_async_copy(out.at[at], out_hbm.at[at], sem.at[step]))
        stores[-1].start()
    for store in stores:
        store.wait()


def finish(*operands):
    return pl.pallas_call(
        finish_kernel,
        in_specs=[pl.BlockSpec(memory_space=pltpu.VMEM)] * 5,
        out_specs=pl.BlockSpec(memory_space=pl.ANY),
        out_shape=jax.ShapeDtypeStruct((ROWS, W), jnp.float32),
        scratch_shapes=[pltpu.VMEM((ROWS, W), jnp.float32), pltpu.SemaphoreType.DMA((6,))],
        compiler_params=pltpu.CompilerParams(vmem_limit_bytes=12 << 20),
        name="finish",
    )(*operands)


def local(q_final, r_first, r_second, q_grad, r_grad):
    return finish(*main(q_final, r_first, r_second, q_grad, r_grad))


def solution(mesh):
    placed = (P("rows", None), P(), P(), P("rows", None), P())
    return jax.shard_map(local, mesh=mesh, in_specs=placed, out_specs=P("rows", None), check_vma=False)
```

```python
import jax
import jax.numpy as jnp
from jax import lax
from jax.experimental import pallas as pl
from jax.experimental.pallas import tpu as pltpu
from jax.sharding import PartitionSpec as P

HIGHEST = lax.Precision.HIGHEST
W, HALF = 512, 256
NX, NY, NZ = 4, 4, 8
ROWS, STEPS = 1536, 3
PARTS = ((0, 4, True), (4, 4, False))
SLOTS = ((0, 5), (5, 9))
FAR_4, FAR_8 = (1, 0, 2), (3, 2, 4, 1, 5, 0, 6)
NN, NT, TN = ((1,), (0,)), ((1,), (1,)), ((0,), (0,))
A, B = slice(0, HALF), slice(HALF, W)


def mm(a, b):
    return lax.dot_general(a, b, (NN, ((), ())), precision=HIGHEST, preferred_element_type=jnp.float32)


def halves(a):
    high = a.astype(jnp.bfloat16)
    return high, (a - high.astype(jnp.float32)).astype(jnp.bfloat16)


def cut(pair, *index):
    return pair[0][index], pair[1][index]


def join(pairs, axis):
    return tuple(jnp.concatenate([p[i] for p in pairs], axis=axis) for i in range(2))


def mm3(a, b, dims=NN):
    (ah, al), (bh, bl) = a, b

    def dot(u, v):
        return lax.dot_general(u, v, (dims, ((), ())), preferred_element_type=jnp.float32)

    return dot(ah, bh) + (dot(ah, bl) + dot(al, bh))


def iotas(rows, cols):
    return lax.broadcasted_iota(jnp.int32, (rows, cols), 0), lax.broadcasted_iota(jnp.int32, (rows, cols), 1)


def small_inverses(uppers, size=128):
    row, col = iotas(size, size)
    eye, above = row == col, col > row
    block = [u[b : b + size, b : b + size] for u in uppers for b in range(0, W, size)]
    inv = []
    for u in block:
        d_row = 1.0 / jnp.sum(jnp.where(eye, u, 0.0), axis=0, keepdims=True)
        d_col = 1.0 / jnp.sum(jnp.where(eye, u, 0.0), axis=1, keepdims=True)
        pair = above & (row // 2 == col // 2)
        inv.append(jnp.where(eye, d_row, jnp.where(pair, -(u * d_col) * d_row, 0.0)))
    s = 2
    while s < size:
        between = above & (row // (2 * s) == col // (2 * s)) & (row // s != col // s)
        half = [mm(jnp.where(between, u, 0.0), x) for u, x in zip(block, inv)]
        inv = [x - mm(x, h) for x, h in zip(inv, half)]
        s *= 2
    return inv


def join_inverses(uppers, outs, size=128):
    s = size
    while s < W:
        for u, out in zip(uppers, outs):
            for b in range(0, W, 2 * s):
                top, low = slice(b, b + s), slice(b + s, b + 2 * s)
                out[top, low] = -mm(out[top, top], mm(u[top, low], out[low, low]))
        s *= 2


def place():
    me = lax.axis_index("rows")
    c = lax.rem(me, 2)
    z = lax.rem(lax.div(me, 2), NZ)
    y = lax.rem(lax.div(me, 2 * NZ), NY)
    x = lax.div(me, 2 * NZ * NY)
    return x, y, z, c


def device(x, y, z, c):
    return (((x * NY + y) * NZ + z) * 2 + c,)


def pack_half(h, wide, square, put):
    row, col = iotas(HALF, HALF)
    low, eye = row >= col, row == col
    is_top = jnp.full((HALF, HALF), h, jnp.int32) == 0
    parts = (jnp.where(low & is_top, square, wide[:, A]), jnp.where(low | is_top, wide[:, B], square))
    diag = jnp.sum(jnp.where(eye, jnp.where(is_top, wide[:, A], square), 0.0), axis=0, keepdims=True)
    first = lax.broadcasted_iota(jnp.int32, (8, 128), 0)
    for group in range(16):
        for tile in range(8):
            r, l = group * 16 + (tile // 4) * 8, (tile % 4) * 128
            put(group // 4, group % 4, tile, parts[l // HALF][r : r + 8, l % HALF : l % HALF + 128])
        extra = jnp.zeros((8, 128), jnp.float32)
        if group == 0:
            lines = [jnp.broadcast_to(diag[:, i * 128 : i * 128 + 128], (8, 128)) for i in range(2)]
            extra = jnp.where(first == 0, lines[0], jnp.where(first == 1, lines[1], 0.0))
        put(group // 4, group % 4, 8, extra)


def copy_lower(m, low, strict):
    return jnp.where(low, m, 0.0) + jnp.where(strict, m, 0.0).T


def symmetric(b00, b10, b11):
    row, col = iotas(HALF, HALF)
    low, strict = row >= col, row > col
    top = jnp.concatenate([copy_lower(b00, low, strict), b10.T], axis=1)
    return jnp.concatenate([top, jnp.concatenate([b10, copy_lower(b11, low, strict)], axis=1)], axis=0)


def middle(square, diag, k1, k2, r2, inv1, inv2, both):
    row, col = iotas(HALF, HALF)
    low, strict, above, eye = row >= col, row > col, row < col, row == col
    second = halves(symmetric(*(k2[i, j] - square[i, j] for i, j in ((A, A), (B, A), (B, B)))))
    grams = []
    for s in (A, B):
        upper = jnp.where(above, square[s, s], 0.0)
        grams.append(upper + upper.T + jnp.where(eye, jnp.broadcast_to(diag[:, s], (HALF, HALF)), 0.0))
    g01 = square[A, B]
    gram_a = halves(jnp.concatenate([grams[0], g01.T], axis=0))
    gram_b = halves(jnp.concatenate([g01, grams[1]], axis=0))
    cross_a = jnp.concatenate([jnp.where(low, square[A, A], 0.0), square[B, A]], axis=0)
    y_a = halves(cross_a + mm3(second, gram_a))
    y_bb = halves(jnp.where(low, square[B, B], 0.0) + mm3(cut(second, B), gram_b))
    w_a = halves(mm3(y_a, cut(r2, A, A)))
    w_bb = halves(mm3(join([cut(y_a, B), y_bb], 1), cut(r2, slice(None), B)))
    z_aa = mm3(cut(inv2, A), w_a)
    z_b = mm3(cut(inv2, B, B), join([cut(w_a, B), w_bb], 1))
    first = halves(symmetric(k1[A, A] - z_aa, k1[B, A] - z_b[:, A], k1[B, B] - z_b[:, B]))
    v = halves(times_lower(first, inv1))
    add = times_lower(second, both)
    return add[A] + mm3(cut(r2, A), v), add[B] + mm3(cut(r2, B, B), cut(v, B))


def times_lower(a, upper):
    return jnp.concatenate([mm3(a, cut(upper, A), NT), mm3(cut(a, slice(None), B), cut(upper, B, B), NT)], axis=1)


def main_kernel(q_hbm, r1_hbm, r2_hbm, g_hbm, rg_hbm, u_buf, slab_h, slab_l, m2_h, m2_l, *scratch):
    scratch = list(scratch)
    q_in, g_in, r1, r2, rg, inv1, inv2, k1, k2, square, diag, acc = (scratch.pop(0) for _ in range(12))
    bf = [scratch.pop(0) for _ in range(8)]
    r2_p, inv1_p, inv2_p, both_p = (tuple(bf[i : i + 2]) for i in range(0, 8, 2))
    theirs, core_in, mine, own, z_in, whole = (scratch.pop(0) for _ in range(6))
    one_in, two, two_in = ([scratch.pop(0) for _ in PARTS] for _ in range(3))
    e_in, lines = scratch.pop(0), scratch.pop(0)
    in_sem, core_sem, one_sem, two_sem, z_sem, four_sem, five_sem, last_sem, e_sem = (scratch.pop(0) for _ in range(9))
    x, y, z, c = place()
    other = device(x, y, z, 1 - c)
    xs = [lax.rem(x + k, NX) for k in range(1, NX)]
    ys = [lax.rem(y + k, NY) for k in range(1, NY)]
    to_x = [device(p, y, z, c) for p in xs]
    to_y = [device(x, p, z, c) for p in ys]
    to_z = [device(x, y, lax.rem(z + k, NZ), c) for k in range(1, NZ)]

    rows = ROWS // STEPS
    loads = []
    for step in range(STEPS):
        at = pl.ds(step * rows, rows)
        for i, (src, dst) in enumerate(((q_hbm, q_in), (g_hbm, g_in))):
            loads.append(pltpu.make_async_copy(src.at[at], dst.at[at], in_sem.at[2 * step + i]))
    for i, (src, dst) in enumerate(((r1_hbm, r1), (r2_hbm, r2), (rg_hbm, rg))):
        loads.append(pltpu.make_async_copy(src, dst, in_sem.at[2 * STEPS + i]))
    for load in loads:
        load.start()

    barrier = pltpu.get_barrier_semaphore()
    peers = [other, *to_x, *to_y, *to_z]
    for peer in peers:
        pl.semaphore_signal(barrier, inc=1, device_id=peer, device_id_type=pl.DeviceIdType.MESH)

    def pair_of(refs):
        return refs[0][...], refs[1][...]

    sent = []

    def send(src, dst, sems, k, to):
        copy = pltpu.make_async_remote_copy(src_ref=src, dst_ref=dst, send_sem=sems.at[0, k], recv_sem=sems.at[1, k],
                                            device_id=to, device_id_type=pl.DeviceIdType.MESH)
        copy.start()
        sent.append(copy)
        return copy

    def gram_half(h, at):
        def slab(i):
            return slab_h[i, at], slab_l[i, at]

        q = join([slab(0), slab(3)], 1)
        return mm3(slab(h), q, TN), mm3(slab(2 + h), slab(3 * h), TN)

    for step in range(STEPS):
        at = slice(step * rows, (step + 1) * rows)
        loads[2 * step].wait()
        loads[2 * step + 1].wait()
        for i, (src, s) in enumerate(((q_in, A), (g_in, B), (g_in, A), (q_in, B))):
            slab_h[i, at], slab_l[i, at] = halves(src[at, s])
        wide, block = gram_half(1 - c, at)
        if step:
            wide, block = acc[:, :W] + wide, acc[:, W:] + block
        if step < STEPS - 1:
            acc[:, :W], acc[:, W:] = wide, block

    def put_theirs(i, j, tile, value):
        theirs[i, j, tile] = value

    pack_half(1 - c, wide, block, put_theirs)
    pl.semaphore_wait(barrier, len(peers))
    core = send(theirs, core_in, core_sem, 0, other)
    wide, block = gram_half(c, slice(None))
    core.wait_recv()

    def put_mine(i, j, tile, value):
        mine[i, j, tile] = value + core_in[i, j, tile]

    pack_half(c, wide, block, put_mine)

    def span(part):
        return pl.ds(part[0], part[1])

    def line(ref, part, at):
        return ref.at[at, :, span(part)] if part[2] else ref.at[:, at, span(part)]

    e_copies = [send(mine.at[0, 0, 8], e_in.at[k], e_sem, k, to_x[k]) for k in FAR_4]
    one = [[send(line(mine, part, (xs if part[2] else ys)[k]), one_in[p].at[k], one_sem, 3 * p + k, (to_x if part[2] else to_y)[k])
            for k in FAR_4] for p, part in enumerate(PARTS)]

    for load in loads[2 * STEPS :]:
        load.wait()
    r2_p[0][...], r2_p[1][...] = halves(r2[...])

    r2_v = pair_of(r2_p)
    r1_v, rg_v = halves(r1[...]), halves(rg[...])
    t = halves(jnp.concatenate([mm3(cut(r1_v, A), rg_v, NT), mm3(cut(r1_v, B, B), cut(rg_v, slice(None), B), NT)], axis=0))
    k2[A, A], k2[B] = mm3(cut(r2_v, A), cut(t, slice(None), A)), mm3(cut(r2_v, B, B), cut(t, B))
    k1[:, A], k1[B, B] = mm3(cut(t, slice(None), A), cut(r2_v, A, A)), mm3(cut(t, B), cut(r2_v, slice(None), B))

    two_copies = []
    for p, part in enumerate(PARTS):
        lo, hi = part[0], part[0] + part[1]
        for copy in one[p]:
            copy.wait_recv()
        here = mine[x, :, lo:hi] if part[2] else mine[:, y, lo:hi]
        two[p][:, 0 : part[1]] = (here + one_in[p][0]) + (one_in[p][1] + one_in[p][2])
        if p == 0:
            for copy in e_copies:
                copy.wait_recv()
            line_sum = (mine[0, 0, 8] + e_in[0]) + (e_in[1] + e_in[2])
            two[p][:, 4] = jnp.broadcast_to(line_sum[None], (4, 8, 128))
        two_copies.append([send(two[p].at[(ys if part[2] else xs)[k]], two_in[p].at[k], two_sem, 3 * p + k, (to_y if part[2] else to_x)[k])
                           for k in FAR_4])

    z_copies = []
    for p, part in enumerate(PARTS):
        lo, hi = SLOTS[p]
        for copy in two_copies[p]:
            copy.wait_recv()
        own[lo:hi] = (two[p][y if part[2] else x] + two_in[p][0]) + (two_in[p][1] + two_in[p][2])
        z_copies.append([send(own.at[pl.ds(lo, hi - lo)], z_in.at[k, pl.ds(lo, hi - lo)], z_sem, 7 * p + k, to_z[k]) for k in FAR_8])

    small = small_inverses((r1[...], r2[...]))
    for m, out in enumerate((inv1, inv2)):
        out[...] = jnp.zeros((W, W), jnp.float32)
        for b in range(4):
            out[b * 128 : b * 128 + 128, b * 128 : b * 128 + 128] = small[4 * m + b]

    join_inverses((r1, r2), (inv1, inv2))
    for pair, ref in ((inv1_p, inv1), (inv2_p, inv2)):
        pair[0][...], pair[1][...] = halves(ref[...])

    i1, i2 = pair_of(inv1_p), pair_of(inv2_p)
    for i, j in ((A, A), (A, B), (B, B)):
        inner = slice(i.start, j.stop)
        both_p[0][i, j], both_p[1][i, j] = halves(mm3(cut(i1, i, inner), cut(i2, inner, j)))
    both_p[0][B, A], both_p[1][B, A] = jnp.zeros((HALF, HALF), jnp.bfloat16), jnp.zeros((HALF, HALF), jnp.bfloat16)
    both = pair_of(both_p)

    four = []
    for p, part in enumerate(PARTS):
        lo, hi = SLOTS[p]
        for copy in z_copies[p]:
            copy.wait_recv()
        total = own[lo:hi]
        for k in range(NZ - 1):
            total = total + z_in[k, lo:hi]
        whole[c, x, y, part[0] : part[0] + part[1]] = total[0 : part[1]]
        if p == 0:
            lines[c] = total[4]
        ref = whole.at[c, x, y, span(part)]
        four.append([send(ref, ref, four_sem, 3 * p + k, (to_y if part[2] else to_x)[k]) for k in FAR_4])
    for step in range(STEPS):
        at = slice(step * rows, (step + 1) * rows)
        g0, g1 = (slab_h[2, at], slab_l[2, at]), (slab_h[1, at], slab_l[1, at])
        u_buf[at, A] = mm3(join([g0, g1], 1), cut(both, A), NT)
        u_buf[at, B] = mm3(g1, cut(both, B, B), NT)

    five = []
    last = [send(lines.at[c], lines.at[c], e_sem, 3, other)]
    mine_all = whole.at[c]
    for p, part in enumerate(PARTS):
        for copy in four[p]:
            copy.wait_recv()
        ref = line(mine_all, part, x if part[2] else y)
        five.append([send(ref, ref, five_sem, 3 * p + k, (to_x if part[2] else to_y)[k]) for k in FAR_4])
        last.append(send(ref, ref, last_sem, 4 * p, other))
    for k in (0, 2, 1):
        for p, part in enumerate(PARTS):
            five[p][FAR_4.index(k)].wait_recv()
            ref = line(mine_all, part, lax.rem((x if part[2] else y) + 3 - k, 4))
            last.append(send(ref, ref, last_sem, 4 * p + 1 + k, other))
    for copy in last:
        copy.wait_recv()

    for group in range(32):
        at = (group // 16, (group // 4) % 4, group % 4)
        for tile in range(8):
            r, l = group * 16 + (tile // 4) * 8, (tile % 4) * 128
            square[r : r + 8, l : l + 128] = whole[(*at, tile)]
    for i in range(4):
        diag[0:1, i * 128 : i * 128 + 128] = lines[i // 2, i % 2 : i % 2 + 1]
    for s, m in zip((A, B), middle(square, diag[0:1], k1, k2, pair_of(r2_p), pair_of(inv1_p), pair_of(inv2_p), pair_of(both_p))):
        m2_h[s], m2_l[s] = halves(m)
    for copy in sent:
        copy.wait_send()


def main(q_final, r_first, r_second, q_grad, r_grad):
    hbm = pl.BlockSpec(memory_space=pl.ANY)
    f32, bf16 = jnp.float32, jnp.bfloat16
    tile = (8, 128)
    scratch = [pltpu.VMEM((ROWS, W), f32)] * 2
    scratch += [pltpu.VMEM((W, W), f32)] * 7
    scratch += [pltpu.VMEM((W, W), f32), pltpu.VMEM((8, W), f32), pltpu.VMEM((HALF, W + HALF), f32)]
    scratch += [pltpu.VMEM((W, W), bf16)] * 8
    scratch += [pltpu.VMEM((NX, NY, 9, *tile), f32)] * 3
    scratch += [pltpu.VMEM((9, *tile), f32), pltpu.VMEM((NZ - 1, 9, *tile), f32), pltpu.VMEM((2, NX, NY, 9, *tile), f32)]
    scratch += [pltpu.VMEM((3, 4, part[1], *tile), f32) for part in PARTS]
    scratch += [pltpu.VMEM((4, hi - lo, *tile), f32) for lo, hi in SLOTS]
    scratch += [pltpu.VMEM((3, hi - lo, *tile), f32) for lo, hi in SLOTS]
    scratch += [pltpu.VMEM((3, *tile), f32), pltpu.VMEM((2, *tile), f32)]
    n = len(PARTS)
    scratch += [pltpu.SemaphoreType.DMA((2 * STEPS + 3,))]
    scratch += [pltpu.SemaphoreType.DMA((2, k)) for k in (1, 3 * n, 3 * n, 7 * n, 3 * n, 3 * n, 4 * n, 4)]
    return pl.pallas_call(
        main_kernel,
        in_specs=[hbm] * 5,
        out_specs=[pl.BlockSpec(memory_space=pltpu.VMEM)] * 5,
        out_shape=[pltpu.VMEM((ROWS, W), f32)] + [pltpu.VMEM((4, ROWS, HALF), bf16)] * 2 + [pltpu.VMEM((W, W), bf16)] * 2,
        scratch_shapes=scratch,
        compiler_params=pltpu.CompilerParams(collective_id=0, has_side_effects=True, vmem_limit_bytes=48 << 20),
        name="main",
    )(q_final, r_first, r_second, q_grad, r_grad)


def finish_kernel(u, slab_h, slab_l, m2_h, m2_l, out_hbm, out, sem):
    m2 = m2_h[...], m2_l[...]
    stores = []
    for step in range(6):
        at = slice(step * 256, (step + 1) * 256)
        q = join([(slab_h[i, at], slab_l[i, at]) for i in (0, 3)], 1)
        out[at] = u[at] + mm3(q, m2)
        stores.append(pltpu.make_async_copy(out.at[at], out_hbm.at[at], sem.at[step]))
        stores[-1].start()
    for store in stores:
        store.wait()


def finish(*operands):
    return pl.pallas_call(
        finish_kernel,
        in_specs=[pl.BlockSpec(memory_space=pltpu.VMEM)] * 5,
        out_specs=pl.BlockSpec(memory_space=pl.ANY),
        out_shape=jax.ShapeDtypeStruct((ROWS, W), jnp.float32),
        scratch_shapes=[pltpu.VMEM((ROWS, W), jnp.float32), pltpu.SemaphoreType.DMA((6,))],
        compiler_params=pltpu.CompilerParams(vmem_limit_bytes=12 << 20),
        name="finish",
    )(*operands)


def local(q_final, r_first, r_second, q_grad, r_grad):
    return finish(*main(q_final, r_first, r_second, q_grad, r_grad))


def solution(mesh):
    placed = (P("rows", None), P(), P(), P("rows", None), P())
    return jax.shard_map(local, mesh=mesh, in_specs=placed, out_specs=P("rows", None), check_vma=False)
```
